32 devices in a mesh: expert: 4 (over z), shard: 8 (over y, x, core).
Axes of the slice: x: 2, y: 2, z: 4, core: 2. Of those that a mesh axis runs over, the one named last changes fastest.
Arguments:
- tokens: bfloat16 [768, 4096], P(('expert', 'shard')), may hold values from -0.19921875 to 0.19921875
- expert_ids: int32 [768, 2], P(('expert', 'shard')), may hold values from 0 to 3, all different within a row; in each aligned block of 24 rows (0 to 23, 24 to 47, ...) at most 16 rows name the same one
- weight_gate: bfloat16 [4, 4096, 8192], P('expert', None, 'shard'), may hold values from -0.09375 to 0.09375
- weight_up: bfloat16 [4, 4096, 8192], P('expert', None, 'shard'), may hold values from -0.09375 to 0.09375
- gate_pre: bfloat16 [4, 512, 8192], P('expert', None, 'shard'), may hold values from -8 to 8
- up_pre: bfloat16 [4, 512, 8192], P('expert', None, 'shard'), may hold values from -6 to 6
- hidden_grad: bfloat16 [4, 512, 8192], P('expert', None, 'shard'), may hold values from -6 to 6
Outputs:
- token_grad: bfloat16 [768, 4096], P(('expert', 'shard'))
- gate_weight_grad: float32 [4, 4096, 8192], P('expert', None, 'shard')
- up_weight_grad: float32 [4, 4096, 8192], P('expert', None, 'shard')
The draws below stay inside these ranges and needn't reach their ends.
Inputs may be any that keep to these rules, and one draw needn't show every extreme that they name: `expert_ids`: each token names 2 different experts. Among the tokens of one device no expert is named more than 16 times, and in every draw some device names some expert exactly 16 times.
All inputs are finite; a program needn't handle non-finite values.
Results may differ from the reference program's by a relative error of at most 0.02.
Values may be sent and summed in bfloat16 or wider, within the bound.
No kernel may reach another device: no remote copies, remote signals or barrier semaphores. Data moves between devices by JAX's collectives and lax.ppermute only.
A program may use at most 192 MiB of HBM per device.

```python
import math
import jax
import jax.numpy as jnp
import numpy as np
from jax import lax

D = 4096
FF = 8192
TOP = 2
TOK_DEV = 24
CAP = 16
EXPERTS = 4
TOKENS = 768
GROUP_ROWS = 512
N_EXPERT = 4
N_SHARD = 8


def shard_levels(rng, dims, split, smallest, high):
    loudness = 1.0
    for dim, shards_of in split:
        steps = jax.random.uniform(jax.random.fold_in(jax.random.fold_in(rng, 6), dim), (shards_of,), jnp.float32, smallest / len(split), high / len(split))
        loudness = loudness * jnp.repeat(jnp.exp(steps), dims[dim] // shards_of).reshape((-1,) + (1,) * (len(dims) - 1 - dim))
    return loudness


def shared_out(own_key, own, number, rows, amount, top, bound, slope):
    sequence = jax.random.permutation(own_key, amount)
    heavy_load, ordinary = load_shares(amount, rows * top, bound, slope, True), load_shares(amount, rows * top, bound, slope, False)
    places = jnp.arange(amount)

    def named(tallies, turn):
        used = int((tallies > 0).sum())
        fixed = max(1, used // 4)
        moved = fixed + (places - fixed + turn * (used - fixed)) % max(1, amount - fixed)
        return jnp.zeros((amount,), jnp.int32).at[sequence[jnp.where(places < fixed, places, moved)]].set(jnp.asarray(tallies, jnp.int32))

    tallies = jnp.where(number % 4 == 0, named(heavy_load, number // 4), named(ordinary, number - number // 4 - 1))
    mixed = jax.random.permutation(jax.random.fold_in(own, 3), amount)
    source_of, receiver = mixed[0:amount // 2 * 2:2], mixed[1:amount // 2 * 2:2]
    slack = jnp.minimum(tallies[source_of] - 1, bound - tallies[receiver]) // 2
    slack = jnp.where((source_of == sequence[0]) | (receiver == sequence[0]) | (tallies[receiver] == 0), 0, jnp.maximum(slack, 0))
    moved = jax.random.randint(jax.random.fold_in(own, 4), (amount // 2,), 0, 1 << 20) % (slack + 1)
    tallies = tallies.at[source_of].add(-moved).at[receiver].add(moved)
    items = jnp.searchsorted(jnp.cumsum(tallies), jnp.arange(rows * top), side="right").astype(jnp.int32)
    listing = items.reshape(top, rows).T
    listing = listing[jax.random.permutation(jax.random.fold_in(own, 1), rows)]
    turn = jax.random.randint(jax.random.fold_in(own, 2), (rows, 1), 0, top)
    return jnp.take_along_axis(listing, (jnp.arange(top)[None, :] + turn) % top, axis=1)


def load_shares(number_of, total, limit, skew, full):
    portions = [(1 << 20) // math.isqrt(standing ** skew) + 1 for standing in range(1, number_of + 1)]
    largest = limit if full else min(limit, max(-(-total // number_of), total * portions[0] // sum(portions)))
    least = 1 if total - largest >= number_of - 1 else 0
    given, surplus = [largest] + [least] * (number_of - 1), total - largest - least * (number_of - 1)
    while surplus > 0:
        free = [i for i in range(1, number_of) if given[i] < largest] or [i for i in range(1, number_of) if given[i] < limit]
        whole, budget = sum([portions[i] for i in free]), surplus
        for i in free:
            addition = min(limit - given[i], max(1, budget * portions[i] // whole), surplus)
            given[i] = given[i] + addition
            surplus = surplus - addition
    return np.array(given)


def centred(key, extent, spread, bound, pieces=(), held_as=jnp.bfloat16):
    gain = shard_levels(key, extent, pieces, -0.22, 0.18) if pieces else 1.0
    drawn = jax.random.normal(key, extent, jnp.float32) * spread * gain
    return jnp.minimum(jnp.maximum(drawn, -bound), bound).astype(held_as)


def setup_inputs(seed: int = 0) -> dict:
    streams_of = jax.random.split(jax.random.key(seed), 8)
    tokens = centred(streams_of[0], (TOKENS, D), 0.03, 0.19921875, ((0, 32),))
    expert_ids_keys = jax.random.split(jax.random.fold_in(streams_of[1], 1), TOKENS // TOK_DEV)
    expert_ids_turns = jax.random.permutation(jax.random.fold_in(streams_of[1], 3), TOKENS // TOK_DEV)
    expert_ids = jax.vmap(lambda own, number: shared_out(jax.random.fold_in(streams_of[1], 2), own, number, TOK_DEV, EXPERTS, TOP, CAP, 2))(expert_ids_keys, expert_ids_turns).reshape((TOKENS, TOP))
    weight_gate = centred(streams_of[2], (EXPERTS, D, FF), D ** -0.5, 0.09375, ((0, 4), (2, 8)))
    weight_up = centred(streams_of[3], (EXPERTS, D, FF), D ** -0.5, 0.09375, ((0, 4), (2, 8)))
    gate_pre = centred(streams_of[4], (EXPERTS, GROUP_ROWS, FF), 1.5, 8.0, ((0, 4), (2, 8)))
    up_pre = centred(streams_of[5], (EXPERTS, GROUP_ROWS, FF), 1.0, 6.0, ((0, 4), (2, 8)))
    hidden_grad = centred(streams_of[6], (EXPERTS, GROUP_ROWS, FF), 1.0, 6.0, ((0, 4), (2, 8)))
    return {"tokens": tokens, "expert_ids": expert_ids, "weight_gate": weight_gate, "weight_up": weight_up, "gate_pre": gate_pre, "up_pre": up_pre, "hidden_grad": hidden_grad}


def swiglu_grads(gate_values, up_values, hidden_cotangent):
    gate_float = gate_values.astype(jnp.float32)
    up_float = up_values.astype(jnp.float32)
    cotangent = hidden_cotangent.astype(jnp.float32)
    sigmoid_gate = jax.nn.sigmoid(gate_float)
    gate_grad = (cotangent * up_float * sigmoid_gate * (1.0 + gate_float * (1.0 - sigmoid_gate))).astype(jnp.bfloat16)
    up_grad = (cotangent * gate_float * sigmoid_gate).astype(jnp.bfloat16)
    return gate_grad, up_grad


def reference(tokens, expert_ids, weight_gate, weight_up, gate_pre, up_pre, hidden_grad):
    devices_all = N_EXPERT * N_SHARD
    width = tokens.shape[1]
    labels = jnp.arange(N_EXPERT, dtype=jnp.int32)
    one_hot = (expert_ids[:, :, None] == labels[None, None, :]).astype(jnp.int32)
    per_device = one_hot.reshape(devices_all, TOK_DEV * TOP, N_EXPERT)
    earlier = jnp.cumsum(per_device, axis=1) - per_device
    slot_index = jnp.sum(per_device * earlier, axis=2).reshape(TOKENS, TOP).astype(jnp.int32)
    token_index = jnp.arange(TOKENS, dtype=jnp.int32)
    device_index = token_index // TOK_DEV
    source_group = device_index // N_SHARD
    source_shard = device_index % N_SHARD
    row_index = ((source_shard * N_EXPERT + source_group)[:, None] * CAP + slot_index).astype(jnp.int32)
    dispatched = jnp.zeros((N_EXPERT, GROUP_ROWS, width), jnp.bfloat16)
    copies = jnp.broadcast_to(tokens[:, None, :], (TOKENS, TOP, width))
    dispatched = dispatched.at[expert_ids, row_index].set(copies)
    block_width = FF // N_SHARD
    gate_wgrads = []
    up_wgrads = []
    slot_grads = []
    for expert in range(N_EXPERT):
        gate_grad, up_grad = swiglu_grads(gate_pre[expert], up_pre[expert], hidden_grad[expert])
        rows_here = dispatched[expert]
        gate_wgrads.append(jnp.dot(rows_here.T, gate_grad, preferred_element_type=jnp.float32))
        up_wgrads.append(jnp.dot(rows_here.T, up_grad, preferred_element_type=jnp.float32))
        gate_matrix = weight_gate[expert]
        up_matrix = weight_up[expert]

        def add_block(total, block_number):
            first_unit = (block_number * block_width).astype(jnp.int32)
            gate_block = lax.dynamic_slice_in_dim(gate_grad, first_unit, block_width, 1)
            up_block = lax.dynamic_slice_in_dim(up_grad, first_unit, block_width, 1)
            gate_weights = lax.dynamic_slice_in_dim(gate_matrix, first_unit, block_width, 1)
            up_weights = lax.dynamic_slice_in_dim(up_matrix, first_unit, block_width, 1)
            block_term = jnp.dot(gate_block, gate_weights.T, preferred_element_type=jnp.float32)
            block_term = block_term + jnp.dot(up_block, up_weights.T, preferred_element_type=jnp.float32)
            return total + block_term.astype(jnp.bfloat16).astype(jnp.float32), None

        start_total = jnp.zeros((GROUP_ROWS, width), jnp.float32)
        total, unused = lax.scan(add_block, start_total, jnp.arange(N_SHARD, dtype=jnp.int32))
        slot_grads.append(total.astype(jnp.bfloat16))
    slot_all = jnp.stack(slot_grads)
    picked = slot_all[expert_ids, row_index].astype(jnp.float32)
    token_grad = jnp.sum(picked, axis=1).astype(jnp.bfloat16)
    return token_grad, jnp.stack(gate_wgrads), jnp.stack(up_wgrads)
```

```python
import functools

import jax
import jax.numpy as jnp
from jax import lax
from jax.experimental import pallas as pl
from jax.experimental.pallas import tpu as pltpu
from jax.sharding import PartitionSpec as P

COLORS = 2


def block_width(width, limit):
    block = min(width, limit)
    while width % block:
        block //= 2
    return block


def slot_table(relative_ids, groups, capacity):
    token_count, choices_per = relative_ids.shape
    labels = lax.broadcasted_iota(jnp.int32, (1, 1, groups), 2)
    one_hot = (relative_ids[:, :, None] == labels).astype(jnp.int32)
    flat_hits = one_hot.reshape(token_count * choices_per, groups)
    earlier = jnp.cumsum(flat_hits, axis=0) - flat_hits
    slot_index = jnp.sum(flat_hits * earlier, axis=1).reshape(token_count, choices_per)
    slot_labels = lax.broadcasted_iota(jnp.int32, (1, 1, 1, capacity), 3)
    slot_hits = one_hot[:, :, :, None] * (slot_index[:, :, None, None] == slot_labels).astype(
        jnp.int32
    )
    selection = jnp.sum(slot_hits, axis=1).reshape(token_count, groups * capacity)
    return selection.astype(jnp.bfloat16)


def swiglu_kernel(place, gate_ref, up_ref, hidden_ref, gate_out, up_out, *, order, groups, capacity):
    expert = place[0]
    shard = place[1]

    def one(source, target):
        a = gate_ref[pl.ds(source, capacity), :].astype(jnp.float32)
        b = up_ref[pl.ds(source, capacity), :].astype(jnp.float32)
        g = hidden_ref[pl.ds(source, capacity), :].astype(jnp.float32)
        sig = 1.0 / (1.0 + jnp.exp(-a))
        gs = g * sig
        gate_out[pl.ds(target, capacity), :] = (gs * b * (1.0 + a * (1.0 - sig))).astype(jnp.bfloat16)
        up_out[pl.ds(target, capacity), :] = (gs * a).astype(jnp.bfloat16)

    for u, mask in enumerate(order):

        def body(k, carry, u=u, mask=mask):
            source = ((shard ^ mask) * groups + lax.rem(expert + k, groups)) * capacity
            target = (u * groups + k) * capacity
            one(pl.multiple_of(source, capacity), pl.multiple_of(target, capacity))
            return carry

        lax.fori_loop(0, groups, body, 0)


def times_transposed(left, right):
    return lax.dot_general(left, right, (((1,), (1,)), ((), ())), preferred_element_type=jnp.float32)


def rows_inner(left, right):
    return lax.dot_general(left, right, (((0,), (0,)), ((), ())), preferred_element_type=jnp.float32)


def dgrad_first(place, gate_pre, up_pre, hidden_grad, weight_gate, weight_up, part, order, groups, capacity):
    rows, units = gate_pre.shape
    width = weight_gate.shape[0] // COLORS
    block = block_width(width, 512)
    steps = width // block

    def kernel(place_ref, gate_ref, up_ref, hidden_ref, wg_ref, wu_ref, gate_out, up_out, out_ref):
        @pl.when(pl.program_id(0) == 0)
        def _():
            swiglu_kernel(
                place_ref, gate_ref, up_ref, hidden_ref, gate_out, up_out,
                order=order, groups=groups, capacity=capacity,
            )

        acc = times_transposed(gate_out[...], wg_ref[...])
        acc = acc + times_transposed(up_out[...], wu_ref[...])
        out_ref[...] = acc.astype(jnp.bfloat16)

    whole = pl.BlockSpec((rows, units), lambda i: (0, 0))
    weight = pl.BlockSpec((block, units), lambda i: (part * steps + i, 0))
    return pl.pallas_call(
        kernel,
        name="dgrad_first",
        grid=(steps,),
        in_specs=[pl.BlockSpec(memory_space=pltpu.SMEM), whole, whole, whole, weight, weight],
        out_specs=[whole, whole, pl.BlockSpec((rows, block), lambda i: (0, i))],
        out_shape=[
            jax.ShapeDtypeStruct((rows, units), jnp.bfloat16),
            jax.ShapeDtypeStruct((rows, units), jnp.bfloat16),
            jax.ShapeDtypeStruct((rows, width), jnp.bfloat16),
        ],
        cost_estimate=pl.CostEstimate(
            flops=4 * rows * units * width, transcendentals=rows * units,
            bytes_accessed=10 * rows * units + 4 * units * width + 2 * rows * width,
        ),
    )(place, gate_pre, up_pre, hidden_grad, weight_gate, weight_up)


def dgrad_more(gate_rows, up_rows, weight_gate, weight_up, part):
    rows, units = gate_rows.shape
    width = weight_gate.shape[0] // COLORS
    block = block_width(width, 512)
    steps = width // block

    def kernel(gate_ref, up_ref, wg_ref, wu_ref, out_ref):
        acc = times_transposed(gate_ref[...], wg_ref[...])
        acc = acc + times_transposed(up_ref[...], wu_ref[...])
        out_ref[...] = acc.astype(jnp.bfloat16)

    whole = pl.BlockSpec((rows, units), lambda i: (0, 0))
    weight = pl.BlockSpec((block, units), lambda i: (part * steps + i, 0))
    return pl.pallas_call(
        kernel,
        name="dgrad_more",
        grid=(steps,),
        in_specs=[whole, whole, weight, weight],
        out_specs=pl.BlockSpec((rows, block), lambda i: (0, i)),
        out_shape=jax.ShapeDtypeStruct((rows, width), jnp.bfloat16),
        cost_estimate=pl.CostEstimate(
            flops=4 * rows * units * width, transcendentals=0,
            bytes_accessed=4 * rows * units + 4 * units * width + 2 * rows * width,
        ),
    )(gate_rows, up_rows, weight_gate, weight_up)


def wgrad(pieces, gate_rows, up_rows):
    rows, units = gate_rows.shape
    count = len(pieces[0])
    piece_rows, width = pieces[0][0].shape
    block = block_width(width, 256)
    steps = width // block

    def kernel(*refs):
        piece_refs = refs[: COLORS * count]
        gate_ref, up_ref, gate_out, up_out = refs[COLORS * count :]

        for color in range(COLORS):

            @pl.when(pl.program_id(0) // steps == color)
            def _(color=color):
                left = jnp.concatenate(
                    [ref[...] for ref in piece_refs[color * count : (color + 1) * count]], axis=0
                )
                gate_out[...] = rows_inner(left, gate_ref[...])
                up_out[...] = rows_inner(left, up_ref[...])

    whole = pl.BlockSpec((rows, units), lambda i: (0, 0))
    out = pl.BlockSpec((block, units), lambda i: (i, 0))

    def piece_spec(color):
        return pl.BlockSpec(
            (piece_rows, block), lambda i: (0, jnp.clip(i - color * steps, 0, steps - 1))
        )

    return pl.pallas_call(
        kernel,
        name="wgrad",
        grid=(COLORS * steps,),
        in_specs=[piece_spec(c) for c in range(COLORS) for _ in range(count)] + [whole, whole],
        out_specs=[out, out],
        out_shape=[jax.ShapeDtypeStruct((COLORS * width, units), jnp.float32)] * 2,
        cost_estimate=pl.CostEstimate(
            flops=4 * rows * units * width * COLORS, transcendentals=0,
            bytes_accessed=4 * rows * units + 2 * COLORS * rows * width + 8 * COLORS * units * width,
        ),
    )(*[p for color in pieces for p in color], gate_rows, up_rows)


def on_device(tokens, expert_ids, weight_gate, weight_up, gate_pre, up_pre, hidden_grad):
    groups = lax.axis_size("expert")
    shards = lax.axis_size("shard")
    expert = lax.axis_index("expert")
    shard = lax.axis_index("shard")
    model_width = tokens.shape[1]
    capacity = gate_pre.shape[1] // (groups * shards)
    half = model_width // COLORS
    bits = [1 << b for b in range(shards.bit_length() - 1)]
    assert 1 << len(bits) == shards
    core, plane = bits[0], bits[1:]
    orders = [plane, plane[::-1]]

    def over_shard(value, bit):
        return lax.ppermute(value, "shard", [(i, i ^ bit) for i in range(shards)])

    def over_expert(value, step):
        return lax.ppermute(value, "expert", [(i, (i + step) % groups) for i in range(groups)])

    order = [0]
    for bit in plane + [core]:
        order = order + [m | bit for m in order]
    axis_of = {bit: n for n, bit in enumerate([core] + plane[::-1])}

    relative_ids = lax.rem(expert - expert_ids + groups, groups)
    selection = slot_table(relative_ids, groups, capacity)
    outgoing = rows_inner(selection, tokens).astype(jnp.bfloat16)
    outgoing = outgoing.reshape(groups, capacity, model_width)
    arrived = [outgoing[0]] + [over_expert(outgoing[k], groups - k) for k in range(1, groups)]
    own = jnp.concatenate(arrived, axis=0)

    place = jnp.stack([expert, shard]).astype(jnp.int32)
    gate_rows, up_rows, first = dgrad_first(
        place, gate_pre[0], up_pre[0], hidden_grad[0], weight_gate[0], weight_up[0],
        0, order, groups, capacity,
    )
    partials = [first] + [
        dgrad_more(gate_rows, up_rows, weight_gate[0], weight_up[0], part)
        for part in range(1, COLORS)
    ]

    summed = []
    for color, partial in enumerate(partials):
        value = partial.reshape((2,) * len(bits) + (groups * capacity, half))
        left = [core] + plane[::-1]
        for bit in [core] + orders[color][::-1]:
            axis = left.index(bit)
            left.remove(bit)
            sent = over_shard(lax.index_in_dim(value, 1, axis, keepdims=False), bit)
            value = lax.index_in_dim(value, 0, axis, keepdims=False) + sent
        summed.append(value)

    pieces = []
    for color in range(COLORS):
        held = {0: own[:, color * half : (color + 1) * half]}
        for bit in orders[color] + [core]:
            held.update({m ^ bit: over_shard(p, bit) for m, p in list(held.items())})
        pieces.append([held[m] for m in order])
    gate_wgrad, up_wgrad = wgrad(pieces, gate_rows, up_rows)

    columns = []
    for value in summed:
        blocks = value.reshape(groups, capacity, half)
        back = [blocks[0]] + [over_expert(blocks[k], k) for k in range(1, groups)]
        returned = jnp.concatenate(back, axis=0)
        columns.append(
            lax.dot_general(
                selection, returned, (((1,), (0,)), ((), ())), preferred_element_type=jnp.float32
            ).astype(jnp.bfloat16)
        )
    token_grad = jnp.concatenate(columns, axis=1)
    return (token_grad, gate_wgrad[None], up_wgrad[None])


def solution(mesh):
    placed = (
        P(("expert", "shard"), None),
        P(("expert", "shard"), None),
        P("expert", None, "shard"),
        P("expert", None, "shard"),
        P("expert", None, "shard"),
        P("expert", None, "shard"),
        P("expert", None, "shard"),
    )
    return jax.shard_map(
        on_device,
        mesh=mesh,
        in_specs=placed,
        out_specs=(
            P(("expert", "shard"), None),
            P("expert", None, "shard"),
            P("expert", None, "shard"),
        ),
        check_vma=False,
    )
```

```python
import jax
import jax.numpy as jnp
from jax import lax
from jax.experimental import pallas as pl
from jax.experimental.pallas import tpu as pltpu
from jax.sharding import PartitionSpec as P


CHUNKS = 2
FUSED = (False, True)
PARTS = 2
DIRECT = (False, True)


def block_width(width, limit):
    block = min(width, limit)
    while width % block:
        block //= 2
    return block


def times_transposed(left, right):
    return lax.dot_general(left, right, (((1,), (1,)), ((), ())), preferred_element_type=jnp.float32)


def rows_inner(left, right):
    return lax.dot_general(left, right, (((0,), (0,)), ((), ())), preferred_element_type=jnp.float32)


def reverse_bits(value, count):
    return sum(((value >> b) & 1) << (count - 1 - b) for b in range(count))


def core_of(place, shards):
    return lax.rem(place[0], shards) & 1


def swiglu_rows(place, shards, gate_ref, up_ref, hidden_ref, gate_out, up_out, plane, groups, capacity):
    count = len(plane)
    expert = lax.div(place[0], shards)
    shard = lax.rem(place[0], shards)
    core = shard & 1
    for v in range(1 << count):
        masks = [
            sum(bits[b] for b in range(count) if (v >> b) & 1) for bits in (plane, plane[::-1])
        ]
        chip = (shard ^ jnp.where(core == 0, masks[0], masks[1])) - core

        def body(n, carry, v=v, chip=chip):
            source = ((chip + lax.rem(n, 2)) * groups + lax.rem(expert + lax.div(n, 2), groups)) * capacity
            target = (v * groups * 2 + n) * capacity
            rows = pl.ds(pl.multiple_of(source, capacity), capacity)
            to = pl.ds(pl.multiple_of(target, capacity), capacity)
            a = gate_ref[rows, :].astype(jnp.float32)
            b = up_ref[rows, :].astype(jnp.float32)
            g = hidden_ref[rows, :].astype(jnp.float32)
            sig = 1.0 / (1.0 + jnp.exp(-a))
            gs = g * sig
            gate_out[to, :] = (gs * b * (1.0 + a * (1.0 - sig))).astype(jnp.bfloat16)
            up_out[to, :] = (gs * a).astype(jnp.bfloat16)
            return carry

        lax.fori_loop(0, groups * 2, body, 0)


def dgrad_cost(rows, units, width, extra):
    return pl.CostEstimate(
        flops=4 * rows * units * width, transcendentals=0,
        bytes_accessed=4 * rows * units + 4 * units * width + 2 * rows * width + extra,
    )


def dgrad_other(place, shards, sources, weight_gate, weight_up, chunks, plane, groups, capacity):
    rows, units = sources[0].shape
    color_width = weight_gate.shape[0] // 2
    width = color_width // chunks
    block = block_width(width, 512)
    steps = width // block
    count = len(plane)
    chip_rows = rows >> count

    def kernel(place_ref, gate_ref, up_ref, hidden_ref, wg_ref, wu_ref, gate_rows, up_rows, *out_refs):
        @pl.when(pl.program_id(0) == 0)
        def _():
            swiglu_rows(
                place_ref, shards, gate_ref, up_ref, hidden_ref, gate_rows, up_rows,
                plane, groups, capacity,
            )

        acc = times_transposed(gate_rows[...], wg_ref[...])
        acc = (acc + times_transposed(up_rows[...], wu_ref[...])).astype(jnp.bfloat16)
        for chunk, out_ref in enumerate(out_refs):

            @pl.when(pl.program_id(0) // steps == chunk)
            def _(out_ref=out_ref):
                for v in range(1 << count):
                    u = reverse_bits(v, count)
                    out_ref[v * chip_rows : (v + 1) * chip_rows, :] = acc[
                        u * chip_rows : (u + 1) * chip_rows, :
                    ]

    whole = pl.BlockSpec((rows, units), lambda i, place_ref: (0, 0))
    weight = pl.BlockSpec(
        (block, units), lambda i, place_ref: ((1 - core_of(place_ref, shards)) * chunks * steps + i, 0)
    )

    def out_spec(chunk):
        return pl.BlockSpec(
            (rows, block), lambda i, place_ref: (0, jnp.clip(i - chunk * steps, 0, steps - 1))
        )

    grads = jax.ShapeDtypeStruct((rows, units), jnp.bfloat16)
    return pl.pallas_call(
        kernel,
        name="dgrad_other",
        grid_spec=pltpu.PrefetchScalarGridSpec(
            num_scalar_prefetch=1,
            grid=(chunks * steps,),
            in_specs=[whole] * 3 + [weight, weight],
            out_specs=[whole, whole] + [out_spec(c) for c in range(chunks)],
        ),
        out_shape=[grads, grads] + [jax.ShapeDtypeStruct((rows, width), jnp.bfloat16)] * chunks,
        cost_estimate=dgrad_cost(rows, units, color_width, 6 * rows * units),
    )(place, *sources, weight_gate, weight_up)


def dgrad_own(place, shards, gate_rows, up_rows, weight_gate, weight_up, chunk, chunks, came):
    rows, units = gate_rows.shape
    width = weight_gate.shape[0] // (2 * chunks)
    block = block_width(width, 512)
    steps = width // block
    middle = rows // 2

    def kernel(place_ref, gate_ref, up_ref, wg_ref, wu_ref, *refs):
        high_ref, low_ref = refs[-2:]
        acc = times_transposed(gate_ref[...], wg_ref[...])
        acc = acc + times_transposed(up_ref[...], wu_ref[...])
        if came:
            acc = acc + refs[0][...].astype(jnp.float32)
        low_ref[...] = acc[:middle].astype(jnp.bfloat16)
        high_ref[...] = acc[middle:].astype(jnp.bfloat16)

    whole = pl.BlockSpec((rows, units), lambda i, place_ref: (0, 0))
    weight = pl.BlockSpec(
        (block, units), lambda i, place_ref: ((core_of(place_ref, shards) * chunks + chunk) * steps + i, 0)
    )
    column = lambda i, place_ref: (0, i)
    return pl.pallas_call(
        kernel,
        grid_spec=pltpu.PrefetchScalarGridSpec(
            num_scalar_prefetch=1,
            grid=(steps,),
            in_specs=[whole, whole, weight, weight] + [pl.BlockSpec((rows, block), column)] * len(came),
            out_specs=[pl.BlockSpec((middle, block), column)] * 2,
        ),
        out_shape=[jax.ShapeDtypeStruct((middle, width), jnp.bfloat16)] * 2,
        cost_estimate=dgrad_cost(rows, units, width, 0),
    )(place, gate_rows, up_rows, weight_gate, weight_up, *came)


def wgrad(place, shards, own_pieces, other_pieces, gate_rows, up_rows, part, parts, into):
    rows, units = gate_rows.shape
    pieces = len(own_pieces)
    piece_rows, width = own_pieces[0].shape
    block = block_width(width, 512)
    steps = width // block

    def kernel(place_ref, *refs):
        gate_ref, up_ref = refs[2 * pieces : 2 * pieces + 2]
        gate_out, up_out, left_ref = refs[-3:]

        def gather(piece_refs):
            for n, ref in enumerate(piece_refs):
                left_ref[n * piece_rows : (n + 1) * piece_rows, :] = ref[...]

        @pl.when(pl.program_id(0) < steps)
        def _():
            gather(refs[:pieces])

        @pl.when(pl.program_id(0) >= steps)
        def _():
            gather(refs[pieces : 2 * pieces])

        gate_out[...] = rows_inner(left_ref[...], gate_ref[...])
        up_out[...] = rows_inner(left_ref[...], up_ref[...])

    def out_index(i, place_ref):
        core = core_of(place_ref, shards)
        color = jnp.where(i < steps, core, 1 - core)
        return ((color * parts + part) * steps + lax.rem(i, steps), 0)

    whole = pl.BlockSpec((rows, units), lambda i, place_ref: (0, 0))
    own = pl.BlockSpec((piece_rows, block), lambda i, place_ref: (0, jnp.minimum(i, steps - 1)))
    other = pl.BlockSpec((piece_rows, block), lambda i, place_ref: (0, jnp.maximum(i - steps, 0)))
    out = pl.BlockSpec((block, units), out_index)
    operands = (place, *own_pieces, *other_pieces, gate_rows, up_rows, *into)
    return pl.pallas_call(
        kernel,
        grid_spec=pltpu.PrefetchScalarGridSpec(
            num_scalar_prefetch=1,
            grid=(2 * steps,),
            in_specs=[own] * pieces
            + [other] * pieces
            + [whole, whole]
            + [pl.BlockSpec(memory_space=pl.ANY)] * len(into),
            out_specs=[out, out],
            scratch_shapes=[pltpu.VMEM((rows, block), jnp.bfloat16)],
        ),
        out_shape=[jax.ShapeDtypeStruct((2 * parts * width, units), jnp.float32)] * 2,
        input_output_aliases={len(operands) - len(into) + n: n for n in range(len(into))},
        cost_estimate=pl.CostEstimate(
            flops=8 * rows * units * width, transcendentals=0,
            bytes_accessed=4 * rows * units + 4 * rows * width + 16 * units * width,
        ),
    )(*operands)


def in_hbm(value):
    return pltpu.with_memory_space_constraint(value, pltpu.HBM)


def total(terms):
    value = terms[0].astype(jnp.float32)
    for term in terms[1:]:
        value = value + term.astype(jnp.float32)
    return value.astype(jnp.bfloat16)


def on_device(tokens, expert_ids, weight_gate, weight_up, gate_pre, up_pre, hidden_grad):
    groups = lax.axis_size("expert")
    shards = lax.axis_size("shard")
    expert = lax.axis_index("expert")
    shard = lax.axis_index("shard")
    token_count, model_width = tokens.shape
    capacity = gate_pre.shape[1] // (groups * shards)
    half = model_width // 2
    width = half // CHUNKS
    bits = [1 << b for b in range(shards.bit_length() - 1)]
    assert 1 << len(bits) == shards
    plane = bits[1:]
    count = len(plane)
    core = shard & 1
    place = (expert * shards + shard).astype(jnp.int32).reshape(1)

    def over_core(value):
        return lax.ppermute(value, "shard", [(i, i ^ 1) for i in range(shards)])

    def over_plane(value, v):
        masks = [
            sum(bits[b] for b in range(count) if (v >> b) & 1) for bits in (plane, plane[::-1])
        ]
        return lax.ppermute(value, "shard", [(i, i ^ masks[i & 1]) for i in range(shards)])

    def over_expert(value, step):
        return lax.ppermute(value, "expert", [(i, (i + step) % groups) for i in range(groups)])

    def by_core(first, second):
        return jnp.where(core == 0, first, second)

    peer_tokens = over_core(tokens)
    peer_ids = over_core(expert_ids)
    both = jnp.concatenate([tokens, peer_tokens], axis=0)
    both = by_core(both[:, :half], both[:, half:])
    both_ids = jnp.concatenate([expert_ids, peer_ids], axis=0)

    relative = lax.rem(expert - both_ids + groups, groups)
    shape = (2 * token_count, groups * 2 * capacity)
    column = lax.broadcasted_iota(jnp.int32, shape, 1)
    token = lax.broadcasted_iota(jnp.int32, shape, 0)
    distance = column // (2 * capacity)
    named = jnp.any(relative[:, :, None] == distance[:, None, :], axis=1)
    named = named & (token // token_count ^ core == column // capacity % 2)
    named = named.astype(jnp.bfloat16)
    square = (2 * token_count, 2 * token_count)
    lower = lax.broadcasted_iota(jnp.int32, square, 0) > lax.broadcasted_iota(jnp.int32, square, 1)
    earlier = lax.dot_general(
        lower.astype(jnp.bfloat16), named, (((1,), (0,)), ((), ())), preferred_element_type=jnp.float32
    )
    selection = jnp.where(earlier == (column % capacity).astype(jnp.float32), named, 0)

    outgoing = rows_inner(selection, both).astype(jnp.bfloat16)
    outgoing = outgoing.reshape(groups, 2 * capacity, half)
    arrived = [outgoing[0]]
    for k in range(1, groups):
        arrived.append(over_expert(outgoing[k], groups - k))

    weights = (weight_gate[0], weight_up[0])
    gate_rows, up_rows, *away = dgrad_other(
        place, shards, (gate_pre[0], up_pre[0], hidden_grad[0]), *weights, CHUNKS,
        plane, groups, capacity,
    )
    came = []
    for chunk in range(CHUNKS):
        came.append(over_core(away[chunk]))
    terms, got = [], []
    for chunk in range(CHUNKS):
        added = (in_hbm(came[chunk]),) if FUSED[chunk] else ()
        high, low = dgrad_own(place, shards, gate_rows, up_rows, *weights, chunk, CHUNKS, added)
        high, low = [high], [low]
        if not added:
            middle = came[chunk].shape[0] // 2
            high.append(came[chunk][middle:])
            low.append(came[chunk][:middle])
        got = over_plane(total(high) if len(high) > 1 else high[0], 1 << count - 1)
        terms.append(low + [got])
    for b in range(count - 1)[::-1]:
        middle = terms[0][0].shape[0] // 2
        sums = [total([t[middle:] for t in chunk_terms]) for chunk_terms in terms]
        joined = over_plane(jnp.concatenate(sums, axis=1), 1 << b)
        terms = [
            [t[:middle] for t in chunk_terms] + [joined[:, c * width : (c + 1) * width]]
            for c, chunk_terms in enumerate(terms)
        ]
    summed = jnp.concatenate([total(chunk_terms) for chunk_terms in terms], axis=1)

    masks = range(1 << count)
    grads = ()
    part_width = half // PARTS
    for part in range(PARTS):
        columns = slice(part * part_width, (part + 1) * part_width)
        held = {0: jnp.concatenate([rows[:, columns] for rows in arrived], axis=0)}
        for v in masks[1:]:
            bit = v if DIRECT[part] else 1 << v.bit_length() - 1
            held[v] = over_plane(held[v ^ bit], bit)
        swapped = {}
        for v in masks:
            swapped[v] = over_core(held[v])
        grads = wgrad(
            place,
            shards,
            [in_hbm(held[v]) for v in masks],
            [in_hbm(swapped[reverse_bits(v, count)]) for v in masks],
            in_hbm(gate_rows),
            in_hbm(up_rows),
            part,
            PARTS,
            grads,
        )
    gate_wgrad, up_wgrad = grads

    blocks = summed.reshape(groups, 2 * capacity, half)
    back = [blocks[0]]
    for k in range(1, groups):
        back.append(over_expert(blocks[k], k))
    combined = lax.dot_general(
        selection, jnp.concatenate(back, axis=0), (((1,), (0,)), ((), ())),
        preferred_element_type=jnp.float32,
    ).astype(jnp.bfloat16)
    kept = combined[:token_count]
    got = over_core(combined[token_count:])
    token_grad = jnp.concatenate([by_core(kept, got), by_core(got, kept)], axis=1)
    return (token_grad, gate_wgrad[None], up_wgrad[None])


def solution(mesh):
    placed = (
        P(("expert", "shard"), None),
        P(("expert", "shard"), None),
        P("expert", None, "shard"),
        P("expert", None, "shard"),
        P("expert", None, "shard"),
        P("expert", None, "shard"),
        P("expert", None, "shard"),
    )

    return jax.shard_map(
        on_device,
        mesh=mesh,
        in_specs=placed,
        out_specs=(
            P(("expert", "shard"), None),
            P("expert", None, "shard"),
            P("expert", None, "shard"),
        ),
        check_vma=False,
    )
```

```python
import jax
import jax.numpy as jnp
from jax import lax
from jax.experimental import pallas as pl
from jax.experimental.pallas import tpu as pltpu
from jax.sharding import PartitionSpec as P


PARTS = 2


def kernel_params(rows):
    mebibytes = 40 if rows <= 512 else 60
    return pltpu.CompilerParams(vmem_limit_bytes=mebibytes * 1024 * 1024)


DIRECT = (False, True)


def block_width(width, limit):
    block = min(width, limit)
    while width % block:
        block //= 2
    return block


def times_transposed(left, right):
    return lax.dot_general(left, right, (((1,), (1,)), ((), ())), preferred_element_type=jnp.float32)


def rows_inner(left, right):
    return lax.dot_general(left, right, (((0,), (0,)), ((), ())), preferred_element_type=jnp.float32)


def reverse_bits(value, count):
    return sum(((value >> b) & 1) << (count - 1 - b) for b in range(count))


def core_of(place, shards):
    return lax.rem(place[0], shards) & 1


def chip_of(place, shards, v, plane):
    count = len(plane)
    shard = lax.rem(place[0], shards)
    core = shard & 1
    masks = [sum(bits[b] for b in range(count) if (v >> b) & 1) for bits in (plane, plane[::-1])]
    return (shard ^ jnp.where(core == 0, masks[0], masks[1])) - core


def swiglu_rows(place, shards, v, source_ref, grads_ref, groups, capacity):
    expert = lax.div(place[0], shards)
    first = v * groups * 2 * capacity

    def body(n, carry):
        source = (lax.rem(n, 2) * groups + lax.rem(expert + lax.div(n, 2), groups)) * capacity
        rows = pl.ds(pl.multiple_of(first + source, capacity), capacity)
        to = pl.ds(pl.multiple_of(first + n * capacity, capacity), capacity)
        a = source_ref[0, rows, :].astype(jnp.float32)
        b = source_ref[1, rows, :].astype(jnp.float32)
        g = source_ref[2, rows, :].astype(jnp.float32)
        sig = 0.5 + 0.5 * jnp.tanh(0.5 * a)
        gs = g * sig
        grads_ref[0, to, :] = (gs * b * (1.0 + a * (1.0 - sig))).astype(jnp.bfloat16)
        grads_ref[1, to, :] = (gs * a).astype(jnp.bfloat16)
        return carry

    lax.fori_loop(0, groups * 2, body, 0)


def dgrad_cost(rows, units, width, extra):
    return pl.CostEstimate(
        flops=4 * rows * units * width, transcendentals=0,
        bytes_accessed=4 * rows * units + 4 * units * width + 2 * rows * width + extra,
    )


def weight_loads(color, wg_ref, wu_ref, weights_ref, sems, block):
    width = weights_ref.shape[1]
    copies = []
    for step in range(width // block):
        first = pl.multiple_of(color * width + step * block, block)
        for n, ref in enumerate((wg_ref, wu_ref)):
            copies.append(
                pltpu.make_async_copy(
                    ref.at[pl.ds(first, block), :],
                    weights_ref.at[n, pl.ds(step * block, block), :],
                    sems.at[2 * step + n],
                )
            )
    return copies


def block_product(grads_ref, weights_ref, loads, step, block):
    acc = None
    for n in range(2):
        loads[2 * step + n].wait()
        for copy in loads[2 * step + n + 2 : 2 * step + n + 3]:
            copy.start()
        term = times_transposed(grads_ref[n], weights_ref[n, step * block : (step + 1) * block, :])
        acc = term if acc is None else acc + term
    return acc


def dgrad_other(place, shards, sources, weight_gate, weight_up, plane, groups, capacity):
    rows, units = sources[0].shape
    width = weight_gate.shape[0] // 2
    block = block_width(width, 512)
    steps = width // block
    count = len(plane)
    chips = 1 << count
    chip_rows = rows // chips

    def kernel(place_ref, *refs):
        source_refs, (wg_ref, wu_ref, gate_out, up_out, out_ref) = refs[:3], refs[3:8]
        source_ref, grads_ref, weights_ref, stage_ref = refs[8:12]
        source_sems, weight_sems, grad_sems, out_sems = refs[12:]
        loads = []
        for v in range(chips):
            chip = chip_of(place_ref, shards, v, plane)
            first = pl.multiple_of(chip * (groups * capacity), chip_rows)
            here = pl.ds(v * chip_rows, chip_rows)
            for n, ref in enumerate(source_refs):
                loads.append(
                    pltpu.make_async_copy(
                        ref.at[pl.ds(first, chip_rows), :],
                        source_ref.at[n, here, :],
                        source_sems.at[3 * v + n],
                    )
                )
        weights = weight_loads(
            1 - core_of(place_ref, shards), wg_ref, wu_ref, weights_ref, weight_sems, block
        )
        for copy in loads:
            copy.start()
        for v in range(chips):
            for copy in loads[3 * v : 3 * v + 3]:
                copy.wait()
            if v == chips - 1:
                for copy in weights[:2]:
                    copy.start()
            swiglu_rows(place_ref, shards, v, source_ref, grads_ref, groups, capacity)
        stores = [
            pltpu.make_async_copy(grads_ref.at[n], out, grad_sems.at[n])
            for n, out in enumerate((gate_out, up_out))
        ]
        for copy in stores:
            copy.start()
        outs = []
        for step in range(steps):
            acc = block_product(grads_ref, weights_ref, weights, step, block).astype(jnp.bfloat16)
            slot = step % 2
            if step >= 2:
                outs[step - 2].wait()
            for v in range(chips):
                u = reverse_bits(v, count)
                stage_ref[slot, v * chip_rows : (v + 1) * chip_rows, :] = acc[
                    u * chip_rows : (u + 1) * chip_rows, :
                ]
            outs.append(
                pltpu.make_async_copy(
                    stage_ref.at[slot], out_ref.at[:, pl.ds(step * block, block)], out_sems.at[slot]
                )
            )
            outs[-1].start()
        for copy in stores + outs[-2:]:
            copy.wait()

    anywhere = pl.BlockSpec(memory_space=pl.ANY)
    grads = jax.ShapeDtypeStruct((rows, units), jnp.bfloat16)
    return pl.pallas_call(
        kernel,
        name="dgrad_other",
        in_specs=[pl.BlockSpec(memory_space=pltpu.SMEM)] + [anywhere] * 5,
        out_specs=[anywhere] * 3,
        scratch_shapes=[
            pltpu.VMEM((3, rows, units), jnp.bfloat16),
            pltpu.VMEM((2, rows, units), jnp.bfloat16),
            pltpu.VMEM((2, width, units), jnp.bfloat16),
            pltpu.VMEM((2, rows, block), jnp.bfloat16),
            pltpu.SemaphoreType.DMA((3 * chips,)),
            pltpu.SemaphoreType.DMA((2 * steps,)),
            pltpu.SemaphoreType.DMA((2,)),
            pltpu.SemaphoreType.DMA((2,)),
        ],
        out_shape=[grads, grads, jax.ShapeDtypeStruct((rows, width), jnp.bfloat16)],
        compiler_params=kernel_params(rows),
        cost_estimate=dgrad_cost(rows, units, width, 6 * rows * units),
    )(place, *[in_hbm(array) for array in (*sources, weight_gate, weight_up)])


def dgrad_own(place, shards, gate_rows, up_rows, weight_gate, weight_up, came):
    rows, units = gate_rows.shape
    width = weight_gate.shape[0] // 2
    block = block_width(width, 512)
    steps = width // block
    middle = rows // 2

    def kernel(place_ref, gate_ref, up_ref, wg_ref, wu_ref, came_ref, *refs):
        high_ref, low_ref, grads_ref, weights_ref, added_ref, stage_ref = refs[:6]
        grad_sems, weight_sems, added_sems, out_sems = refs[6:]
        grads = [
            pltpu.make_async_copy(ref, grads_ref.at[n], grad_sems.at[n])
            for n, ref in enumerate((gate_ref, up_ref))
        ]
        weights = weight_loads(
            core_of(place_ref, shards), wg_ref, wu_ref, weights_ref, weight_sems, block
        )
        added = [
            pltpu.make_async_copy(
                came_ref.at[:, pl.ds(step * block, block)], added_ref.at[step % 2], added_sems.at[step % 2]
            )
            for step in range(steps)
        ]
        for copy in [grads[0], weights[0], grads[1], weights[1], *added[:2]]:
            copy.start()
        for copy in grads:
            copy.wait()
        outs = []
        for step in range(steps):
            slot = step % 2
            acc = block_product(grads_ref, weights_ref, weights, step, block)
            added[step].wait()
            if step >= 2:
                for copy in outs[step - 2]:
                    copy.wait()
            stage_ref[slot] = (acc + added_ref[slot].astype(jnp.float32)).astype(jnp.bfloat16)
            if step + 2 < steps:
                added[step + 2].start()
            columns = pl.ds(step * block, block)
            outs.append([
                pltpu.make_async_copy(
                    stage_ref.at[slot, pl.ds(part * middle, middle), :],
                    ref.at[:, columns],
                    out_sems.at[2 * slot + part],
                )
                for part, ref in enumerate((low_ref, high_ref))
            ])
            for copy in outs[-1]:
                copy.start()
        for copies in outs[-2:]:
            for copy in copies:
                copy.wait()

    anywhere = pl.BlockSpec(memory_space=pl.ANY)
    return pl.pallas_call(
        kernel,
        name="dgrad_own",
        in_specs=[pl.BlockSpec(memory_space=pltpu.SMEM)] + [anywhere] * 5,
        out_specs=[anywhere] * 2,
        scratch_shapes=[
            pltpu.VMEM((2, rows, units), jnp.bfloat16),
            pltpu.VMEM((2, width, units), jnp.bfloat16),
            pltpu.VMEM((2, rows, block), jnp.bfloat16),
            pltpu.VMEM((2, rows, block), jnp.bfloat16),
            pltpu.SemaphoreType.DMA((2,)),
            pltpu.SemaphoreType.DMA((2 * steps,)),
            pltpu.SemaphoreType.DMA((2,)),
            pltpu.SemaphoreType.DMA((4,)),
        ],
        out_shape=[jax.ShapeDtypeStruct((middle, width), jnp.bfloat16)] * 2,
        compiler_params=kernel_params(rows),
        cost_estimate=dgrad_cost(rows, units, width, 2 * rows * width),
    )(place, gate_rows, up_rows, in_hbm(weight_gate), in_hbm(weight_up), came)


def in_hbm(value):
    return pltpu.with_memory_space_constraint(value, pltpu.HBM)


def wgrad(place, shards, own_pieces, other_pieces, gate_rows, up_rows, part, parts, into):
    rows, units = gate_rows.shape
    pieces = len(own_pieces)
    piece_rows, width = own_pieces[0].shape
    block = block_width(width, 512)
    steps = width // block
    slots = 4

    def kernel(place_ref, *refs):
        gate_ref, up_ref = refs[2 * pieces : 2 * pieces + 2]
        gate_out, up_out, left_ref, grads_ref, slot_ref, in_sems, out_sems = refs[-7:]
        core = core_of(place_ref, shards)

        def load(n, source, target):
            return pltpu.make_async_copy(source, target, in_sems.at[n])

        grads_in = [load(n, ref, grads_ref.at[n]) for n, ref in enumerate((gate_ref, up_ref))]
        left_in = [
            load(2 + n, ref, left_ref.at[n // pieces, pl.ds(n % pieces * piece_rows, piece_rows), :])
            for n, ref in enumerate(refs[: 2 * pieces])
        ]
        for copy in grads_in[:1] + left_in[:pieces]:
            copy.start()
        stores = []
        for color in range(2):
            for copy in left_in[color * pieces : (color + 1) * pieces]:
                copy.wait()
            where = jnp.where(color == 0, core, 1 - core) * parts + part
            for step in range(steps):
                for n, out in enumerate((gate_out, up_out)):
                    if color == 0 and step == 0:
                        grads_in[n].wait()
                        if n == 0:
                            for copy in grads_in[1:] + left_in[pieces:]:
                                copy.start()
                    slot = len(stores) % slots
                    if len(stores) >= slots:
                        stores[-slots].wait()
                    slot_ref[slot] = rows_inner(
                        left_ref[color, :, step * block : (step + 1) * block], grads_ref[n]
                    )
                    first = pl.multiple_of((where * steps + step) * block, block)
                    stores.append(
                        pltpu.make_async_copy(
                            slot_ref.at[slot], out.at[pl.ds(first, block), :], out_sems.at[slot]
                        )
                    )
                    stores[-1].start()
        for copy in stores[-slots:]:
            copy.wait()

    operands = (place, *own_pieces, *other_pieces, gate_rows, up_rows, *into)
    anywhere = pl.BlockSpec(memory_space=pl.ANY)
    return pl.pallas_call(
        kernel,
        in_specs=[pl.BlockSpec(memory_space=pltpu.SMEM)] + [anywhere] * (len(operands) - 1),
        out_specs=[anywhere] * 2,
        scratch_shapes=[
            pltpu.VMEM((2, rows, width), jnp.bfloat16),
            pltpu.VMEM((2, rows, units), jnp.bfloat16),
            pltpu.VMEM((slots, block, units), jnp.float32),
            pltpu.SemaphoreType.DMA((2 + 2 * pieces,)),
            pltpu.SemaphoreType.DMA((slots,)),
        ],
        out_shape=[jax.ShapeDtypeStruct((2 * parts * width, units), jnp.float32)] * 2,
        input_output_aliases={len(operands) - len(into) + n: n for n in range(len(into))},
        compiler_params=kernel_params(rows),
        cost_estimate=pl.CostEstimate(
            flops=8 * rows * units * width, transcendentals=0,
            bytes_accessed=4 * rows * units + 4 * rows * width + 16 * units * width,
        ),
    )(*operands)


def total(terms):
    value = terms[0].astype(jnp.float32)
    for term in terms[1:]:
        value = value + term.astype(jnp.float32)
    return value.astype(jnp.bfloat16)


def on_device(tokens, expert_ids, weight_gate, weight_up, gate_pre, up_pre, hidden_grad):
    groups = lax.axis_size("expert")
    shards = lax.axis_size("shard")
    expert = lax.axis_index("expert")
    shard = lax.axis_index("shard")
    token_count, model_width = tokens.shape
    capacity = gate_pre.shape[1] // (groups * shards)
    half = model_width // 2
    bits = [1 << b for b in range(shards.bit_length() - 1)]
    assert 1 << len(bits) == shards
    plane = bits[1:]
    count = len(plane)
    core = shard & 1
    place = (expert * shards + shard).astype(jnp.int32).reshape(1)

    def over_core(value):
        return lax.ppermute(value, "shard", [(i, i ^ 1) for i in range(shards)])

    def over_plane(value, v):
        masks = [
            sum(bits[b] for b in range(count) if (v >> b) & 1) for bits in (plane, plane[::-1])
        ]
        return lax.ppermute(value, "shard", [(i, i ^ masks[i & 1]) for i in range(shards)])

    def over_expert(value, step):
        return lax.ppermute(value, "expert", [(i, (i + step) % groups) for i in range(groups)])

    def by_core(first, second):
        return jnp.where(core == 0, first, second)

    peer_tokens = over_core(tokens)
    peer_ids = over_core(expert_ids)
    both = jnp.concatenate([tokens, peer_tokens], axis=0)
    both = by_core(both[:, :half], both[:, half:])
    both_ids = jnp.concatenate([expert_ids, peer_ids], axis=0)

    relative = lax.rem(expert - both_ids + groups, groups)
    shape = (2 * token_count, groups * 2 * capacity)
    column = lax.broadcasted_iota(jnp.int32, shape, 1)
    token = lax.broadcasted_iota(jnp.int32, shape, 0)
    distance = column // (2 * capacity)
    named = jnp.any(relative[:, :, None] == distance[:, None, :], axis=1)
    named = named & (token // token_count ^ core == column // capacity % 2)
    named = named.astype(jnp.bfloat16)
    square = (2 * token_count, 2 * token_count)
    lower = lax.broadcasted_iota(jnp.int32, square, 0) > lax.broadcasted_iota(jnp.int32, square, 1)
    earlier = lax.dot_general(
        lower.astype(jnp.bfloat16), named, (((1,), (0,)), ((), ())), preferred_element_type=jnp.float32
    )
    selection = jnp.where(earlier == (column % capacity).astype(jnp.float32), named, 0)

    outgoing = rows_inner(selection, both).astype(jnp.bfloat16)
    outgoing = outgoing.reshape(groups, 2 * capacity, half)
    arrived = [outgoing[0]]
    for k in range(1, groups):
        arrived.append(over_expert(outgoing[k], groups - k))

    weights = (weight_gate[0], weight_up[0])
    gate_rows, up_rows, away = dgrad_other(
        place, shards, (gate_pre[0], up_pre[0], hidden_grad[0]), *weights, plane, groups, capacity
    )
    came = over_core(away)
    high, low = dgrad_own(place, shards, gate_rows, up_rows, *weights, came)
    terms = [low]
    for b in range(count)[::-1]:
        if b < count - 1:
            middle = terms[0].shape[0] // 2
            high = total([t[middle:] for t in terms])
            terms = [t[:middle] for t in terms]
        terms.append(over_plane(high, 1 << b))
    summed = total(terms)

    masks = range(1 << count)
    grads = ()
    part_width = half // PARTS
    for part in range(PARTS):
        columns = slice(part * part_width, (part + 1) * part_width)
        held = {0: jnp.concatenate([rows[:, columns] for rows in arrived], axis=0)}
        for v in masks[1:]:
            bit = v if DIRECT[part] else 1 << v.bit_length() - 1
            held[v] = over_plane(held[v ^ bit], bit)
        swapped = {}
        for v in masks:
            swapped[v] = over_core(held[v])
        grads = wgrad(
            place,
            shards,
            [held[v] for v in masks],
            [swapped[reverse_bits(v, count)] for v in masks],
            gate_rows,
            up_rows,
            part,
            PARTS,
            grads,
        )
    gate_wgrad, up_wgrad = grads

    blocks = summed.reshape(groups, 2 * capacity, half)
    back = [blocks[0]]
    for k in range(1, groups):
        back.append(over_expert(blocks[k], k))
    combined = lax.dot_general(
        selection, jnp.concatenate(back, axis=0), (((1,), (0,)), ((), ())),
        preferred_element_type=jnp.float32,
    ).astype(jnp.bfloat16)
    kept = combined[:token_count]
    got = over_core(combined[token_count:])
    token_grad = jnp.concatenate([by_core(kept, got), by_core(got, kept)], axis=1)
    return (token_grad, gate_wgrad[None], up_wgrad[None])


def solution(mesh):
    placed = (
        P(("expert", "shard"), None),
        P(("expert", "shard"), None),
        P("expert", None, "shard"),
        P("expert", None, "shard"),
        P("expert", None, "shard"),
        P("expert", None, "shard"),
        P("expert", None, "shard"),
    )

    return jax.shard_map(
        on_device,
        mesh=mesh,
        in_specs=placed,
        out_specs=(
            P(("expert", "shard"), None),
            P("expert", None, "shard"),
            P("expert", None, "shard"),
        ),
        check_vma=False,
    )
```

```python
import jax
import jax.numpy as jnp
from jax import lax
from jax.experimental import pallas as pl
from jax.experimental.pallas import tpu as pltpu
from jax.sharding import PartitionSpec as P


PARTS = 2


def kernel_params(rows):
    mebibytes = 40 if rows <= 512 else 60
    return pltpu.CompilerParams(vmem_limit_bytes=mebibytes * 1024 * 1024)


DIRECT = (False, False)


def block_width(width, limit):
    block = min(width, limit)
    while width % block:
        block //= 2
    return block


def times_transposed(left, right):
    return lax.dot_general(left, right, (((1,), (1,)), ((), ())), preferred_element_type=jnp.float32)


def rows_inner(left, right):
    return lax.dot_general(left, right, (((0,), (0,)), ((), ())), preferred_element_type=jnp.float32)


def reverse_bits(value, count):
    return sum(((value >> b) & 1) << (count - 1 - b) for b in range(count))


def core_of(place, shards):
    return lax.rem(place[0], shards) & 1


def chip_of(place, shards, v, plane):
    count = len(plane)
    shard = lax.rem(place[0], shards)
    core = shard & 1
    masks = [sum(bits[b] for b in range(count) if (v >> b) & 1) for bits in (plane, plane[::-1])]
    return (shard ^ jnp.where(core == 0, masks[0], masks[1])) - core


def swiglu_rows(place, shards, v, source_ref, grads_ref, groups, capacity):
    expert = lax.div(place[0], shards)
    first = v * groups * 2 * capacity

    def body(n, carry):
        source = (lax.rem(n, 2) * groups + lax.rem(expert + lax.div(n, 2), groups)) * capacity
        rows = pl.ds(pl.multiple_of(first + source, capacity), capacity)
        to = pl.ds(pl.multiple_of(first + n * capacity, capacity), capacity)
        a = source_ref[0, rows, :].astype(jnp.float32)
        b = source_ref[1, rows, :].astype(jnp.float32)
        g = source_ref[2, rows, :].astype(jnp.float32)
        sig = 0.5 + 0.5 * jnp.tanh(0.5 * a)
        gs = g * sig
        grads_ref[0, to, :] = (gs * b * (1.0 + a * (1.0 - sig))).astype(jnp.bfloat16)
        grads_ref[1, to, :] = (gs * a).astype(jnp.bfloat16)
        return carry

    lax.fori_loop(0, groups * 2, body, 0)


def dgrad_cost(rows, units, width, extra):
    return pl.CostEstimate(
        flops=4 * rows * units * width, transcendentals=0,
        bytes_accessed=4 * rows * units + 4 * units * width + 2 * rows * width + extra,
    )


def weight_loads(color, wg_ref, wu_ref, weights_ref, sems, block):
    width = weights_ref.shape[1]
    copies = []
    for step in range(width // block):
        first = pl.multiple_of(color * width + step * block, block)
        for n, ref in enumerate((wg_ref, wu_ref)):
            copies.append(
                pltpu.make_async_copy(
                    ref.at[pl.ds(first, block), :],
                    weights_ref.at[n, pl.ds(step * block, block), :],
                    sems.at[2 * step + n],
                )
            )
    return copies


def block_product(grads_ref, weights_ref, loads, step, block, ready=()):
    acc = None
    for n in range(2):
        for copy in ready[n : n + 1]:
            copy.wait()
        loads[2 * step + n].wait()
        for copy in loads[2 * step + n + 2 : 2 * step + n + 3]:
            copy.start()
        term = times_transposed(grads_ref[n], weights_ref[n, step * block : (step + 1) * block, :])
        acc = term if acc is None else acc + term
    return acc


def dgrad_other(place, shards, sources, weight_gate, weight_up, plane, groups, capacity):
    rows, units = sources[0].shape
    width = weight_gate.shape[0] // 2
    block = block_width(width, 512)
    steps = width // block
    count = len(plane)
    chips = 1 << count
    chip_rows = rows // chips

    def kernel(place_ref, *refs):
        source_refs, (wg_ref, wu_ref, gate_out, up_out, out_ref) = refs[:3], refs[3:8]
        source_ref, grads_ref, weights_ref, stage_ref = refs[8:12]
        source_sems, weight_sems, grad_sems, out_sems = refs[12:]
        loads = []
        for v in range(chips):
            chip = chip_of(place_ref, shards, v, plane)
            first = pl.multiple_of(chip * (groups * capacity), chip_rows)
            here = pl.ds(v * chip_rows, chip_rows)
            for n, ref in enumerate(source_refs):
                loads.append(
                    pltpu.make_async_copy(
                        ref.at[pl.ds(first, chip_rows), :],
                        source_ref.at[n, here, :],
                        source_sems.at[3 * v + n],
                    )
                )
        weights = weight_loads(
            1 - core_of(place_ref, shards), wg_ref, wu_ref, weights_ref, weight_sems, block
        )
        for copy in loads:
            copy.start()
        for v in range(chips):
            for copy in loads[3 * v : 3 * v + 3]:
                copy.wait()
            if v == 0:
                for copy in weights[:2]:
                    copy.start()
            swiglu_rows(place_ref, shards, v, source_ref, grads_ref, groups, capacity)
        stores = [
            pltpu.make_async_copy(grads_ref.at[n], out, grad_sems.at[n])
            for n, out in enumerate((gate_out, up_out))
        ]
        for copy in stores:
            copy.start()
        outs = []
        for step in range(steps):
            acc = block_product(grads_ref, weights_ref, weights, step, block).astype(jnp.bfloat16)
            slot = step % 2
            if step >= 2:
                outs[step - 2].wait()
            for v in range(chips):
                u = reverse_bits(v, count)
                stage_ref[slot, v * chip_rows : (v + 1) * chip_rows, :] = acc[
                    u * chip_rows : (u + 1) * chip_rows, :
                ]
            outs.append(
                pltpu.make_async_copy(
                    stage_ref.at[slot], out_ref.at[:, pl.ds(step * block, block)], out_sems.at[slot]
                )
            )
            outs[-1].start()
        for copy in stores + outs[-2:]:
            copy.wait()

    anywhere = pl.BlockSpec(memory_space=pl.ANY)
    grads = jax.ShapeDtypeStruct((rows, units), jnp.bfloat16)
    return pl.pallas_call(
        kernel,
        name="dgrad_other",
        in_specs=[pl.BlockSpec(memory_space=pltpu.SMEM)] + [anywhere] * 5,
        out_specs=[anywhere] * 3,
        scratch_shapes=[
            pltpu.VMEM((3, rows, units), jnp.bfloat16),
            pltpu.VMEM((2, rows, units), jnp.bfloat16),
            pltpu.VMEM((2, width, units), jnp.bfloat16),
            pltpu.VMEM((2, rows, block), jnp.bfloat16),
            pltpu.SemaphoreType.DMA((3 * chips,)),
            pltpu.SemaphoreType.DMA((2 * steps,)),
            pltpu.SemaphoreType.DMA((2,)),
            pltpu.SemaphoreType.DMA((2,)),
        ],
        out_shape=[grads, grads, jax.ShapeDtypeStruct((rows, width), jnp.bfloat16)],
        compiler_params=kernel_params(rows),
        cost_estimate=dgrad_cost(rows, units, width, 6 * rows * units),
    )(place, *[in_hbm(array) for array in (*sources, weight_gate, weight_up)])


def dgrad_own(place, shards, gate_rows, up_rows, weight_gate, weight_up, came):
    rows, units = gate_rows.shape
    width = weight_gate.shape[0] // 2
    block = block_width(width, 512)
    steps = width // block
    middle = rows // 2

    def kernel(place_ref, gate_ref, up_ref, wg_ref, wu_ref, came_ref, *refs):
        high_ref, low_ref, grads_ref, weights_ref, added_ref, stage_ref = refs[:6]
        grad_sems, weight_sems, added_sems, out_sems = refs[6:]
        grads = [
            pltpu.make_async_copy(ref, grads_ref.at[n], grad_sems.at[n])
            for n, ref in enumerate((gate_ref, up_ref))
        ]
        weights = weight_loads(
            core_of(place_ref, shards), wg_ref, wu_ref, weights_ref, weight_sems, block
        )
        added = [
            pltpu.make_async_copy(
                came_ref.at[:, pl.ds(step * block, block)], added_ref.at[step % 2], added_sems.at[step % 2]
            )
            for step in range(steps)
        ]
        for copy in [grads[0], weights[0], grads[1], weights[1], *added[:2]]:
            copy.start()
        outs = []
        for step in range(steps):
            slot = step % 2
            ready = grads if step == 0 else ()
            acc = block_product(grads_ref, weights_ref, weights, step, block, ready)
            added[step].wait()
            if step >= 2:
                for copy in outs[step - 2]:
                    copy.wait()
            stage_ref[slot] = (acc + added_ref[slot].astype(jnp.float32)).astype(jnp.bfloat16)
            if step + 2 < steps:
                added[step + 2].start()
            columns = pl.ds(step * block, block)
            outs.append([
                pltpu.make_async_copy(
                    stage_ref.at[slot, pl.ds(part * middle, middle), :],
                    ref.at[:, columns],
                    out_sems.at[2 * slot + part],
                )
                for part, ref in enumerate((low_ref, high_ref))
            ])
            for copy in outs[-1]:
                copy.start()
        for copies in outs[-2:]:
            for copy in copies:
                copy.wait()

    anywhere = pl.BlockSpec(memory_space=pl.ANY)
    return pl.pallas_call(
        kernel,
        name="dgrad_own",
        in_specs=[pl.BlockSpec(memory_space=pltpu.SMEM)] + [anywhere] * 5,
        out_specs=[anywhere] * 2,
        scratch_shapes=[
            pltpu.VMEM((2, rows, units), jnp.bfloat16),
            pltpu.VMEM((2, width, units), jnp.bfloat16),
            pltpu.VMEM((2, rows, block), jnp.bfloat16),
            pltpu.VMEM((2, rows, block), jnp.bfloat16),
            pltpu.SemaphoreType.DMA((2,)),
            pltpu.SemaphoreType.DMA((2 * steps,)),
            pltpu.SemaphoreType.DMA((2,)),
            pltpu.SemaphoreType.DMA((4,)),
        ],
        out_shape=[jax.ShapeDtypeStruct((middle, width), jnp.bfloat16)] * 2,
        compiler_params=kernel_params(rows),
        cost_estimate=dgrad_cost(rows, units, width, 2 * rows * width),
    )(place, gate_rows, up_rows, in_hbm(weight_gate), in_hbm(weight_up), came)


def in_hbm(value):
    return pltpu.with_memory_space_constraint(value, pltpu.HBM)


def wgrad(place, shards, own_pieces, other_pieces, gate_rows, up_rows, part, parts, into):
    rows, units = gate_rows.shape
    pieces = len(own_pieces)
    piece_rows, width = own_pieces[0].shape
    block = block_width(width, 512)
    steps = width // block
    slots = 4

    def kernel(place_ref, *refs):
        gate_ref, up_ref = refs[2 * pieces : 2 * pieces + 2]
        gate_out, up_out, left_ref, grads_ref, slot_ref, in_sems, out_sems = refs[-7:]
        core = core_of(place_ref, shards)

        def load(n, source, target):
            return pltpu.make_async_copy(source, target, in_sems.at[n])

        grads_in = [load(n, ref, grads_ref.at[n]) for n, ref in enumerate((gate_ref, up_ref))]
        left_in = [
            load(2 + n, ref, left_ref.at[n // pieces, pl.ds(n % pieces * piece_rows, piece_rows), :])
            for n, ref in enumerate(refs[: 2 * pieces])
        ]
        for copy in grads_in[:1] + left_in[:pieces]:
            copy.start()
        stores = []
        for color in range(2):
            for copy in left_in[color * pieces : (color + 1) * pieces]:
                copy.wait()
            where = jnp.where(color == 0, core, 1 - core) * parts + part
            for step in range(steps):
                for n, out in enumerate((gate_out, up_out)):
                    if color == 0 and step == 0:
                        grads_in[n].wait()
                        if n == 0:
                            for copy in grads_in[1:] + left_in[pieces:]:
                                copy.start()
                    slot = len(stores) % slots
                    if len(stores) >= slots:
                        stores[-slots].wait()
                    slot_ref[slot] = rows_inner(
                        left_ref[color, :, step * block : (step + 1) * block], grads_ref[n]
                    )
                    first = pl.multiple_of((where * steps + step) * block, block)
                    stores.append(
                        pltpu.make_async_copy(
                            slot_ref.at[slot], out.at[pl.ds(first, block), :], out_sems.at[slot]
                        )
                    )
                    stores[-1].start()
        for copy in stores[-slots:]:
            copy.wait()

    operands = (place, *own_pieces, *other_pieces, gate_rows, up_rows, *into)
    anywhere = pl.BlockSpec(memory_space=pl.ANY)
    return pl.pallas_call(
        kernel,
        in_specs=[pl.BlockSpec(memory_space=pltpu.SMEM)] + [anywhere] * (len(operands) - 1),
        out_specs=[anywhere] * 2,
        scratch_shapes=[
            pltpu.VMEM((2, rows, width), jnp.bfloat16),
            pltpu.VMEM((2, rows, units), jnp.bfloat16),
            pltpu.VMEM((slots, block, units), jnp.float32),
            pltpu.SemaphoreType.DMA((2 + 2 * pieces,)),
            pltpu.SemaphoreType.DMA((slots,)),
        ],
        out_shape=[jax.ShapeDtypeStruct((2 * parts * width, units), jnp.float32)] * 2,
        input_output_aliases={len(operands) - len(into) + n: n for n in range(len(into))},
        compiler_params=kernel_params(rows),
        cost_estimate=pl.CostEstimate(
            flops=8 * rows * units * width, transcendentals=0,
            bytes_accessed=4 * rows * units + 4 * rows * width + 16 * units * width,
        ),
    )(*operands)


def total(terms):
    value = terms[0].astype(jnp.float32)
    for term in terms[1:]:
        value = value + term.astype(jnp.float32)
    return value.astype(jnp.bfloat16)


def on_device(tokens, expert_ids, weight_gate, weight_up, gate_pre, up_pre, hidden_grad):
    groups = lax.axis_size("expert")
    shards = lax.axis_size("shard")
    expert = lax.axis_index("expert")
    shard = lax.axis_index("shard")
    token_count, model_width = tokens.shape
    capacity = gate_pre.shape[1] // (groups * shards)
    half = model_width // 2
    bits = [1 << b for b in range(shards.bit_length() - 1)]
    assert 1 << len(bits) == shards
    plane = bits[1:]
    count = len(plane)
    core = shard & 1
    place = (expert * shards + shard).astype(jnp.int32).reshape(1)

    def over_core(value):
        return lax.ppermute(value, "shard", [(i, i ^ 1) for i in range(shards)])

    def over_plane(value, v):
        masks = [
            sum(bits[b] for b in range(count) if (v >> b) & 1) for bits in (plane, plane[::-1])
        ]
        return lax.ppermute(value, "shard", [(i, i ^ masks[i & 1]) for i in range(shards)])

    def over_expert(value, step):
        return lax.ppermute(value, "expert", [(i, (i + step) % groups) for i in range(groups)])

    def by_core(first, second):
        return jnp.where(core == 0, first, second)

    peer_tokens = over_core(tokens)
    peer_ids = over_core(expert_ids)
    both = jnp.concatenate([tokens, peer_tokens], axis=0)
    both = by_core(both[:, :half], both[:, half:])
    both_ids = jnp.concatenate([expert_ids, peer_ids], axis=0)

    relative = lax.rem(expert - both_ids + groups, groups)
    shape = (2 * token_count, groups * 2 * capacity)
    column = lax.broadcasted_iota(jnp.int32, shape, 1)
    token = lax.broadcasted_iota(jnp.int32, shape, 0)
    distance = column // (2 * capacity)
    named = jnp.any(relative[:, :, None] == distance[:, None, :], axis=1)
    named = named & (token // token_count ^ core == column // capacity % 2)
    named = named.astype(jnp.bfloat16)
    square = (2 * token_count, 2 * token_count)
    lower = lax.broadcasted_iota(jnp.int32, square, 0) > lax.broadcasted_iota(jnp.int32, square, 1)
    earlier = lax.dot_general(
        lower.astype(jnp.bfloat16), named, (((1,), (0,)), ((), ())), preferred_element_type=jnp.float32
    )
    selection = jnp.where(earlier == (column % capacity).astype(jnp.float32), named, 0)

    outgoing = rows_inner(selection, both).astype(jnp.bfloat16)
    outgoing = outgoing.reshape(groups, 2 * capacity, half)
    arrived = [outgoing[0]]
    for k in range(1, groups):
        arrived.append(over_expert(outgoing[k], groups - k))

    weights = (weight_gate[0], weight_up[0])
    gate_rows, up_rows, away = dgrad_other(
        place, shards, (gate_pre[0], up_pre[0], hidden_grad[0]), *weights, plane, groups, capacity
    )
    came = over_core(away)
    high, low = dgrad_own(place, shards, gate_rows, up_rows, *weights, came)
    terms = [low]
    for b in range(count)[::-1]:
        if b < count - 1:
            middle = terms[0].shape[0] // 2
            high = total([t[middle:] for t in terms])
            terms = [t[:middle] for t in terms]
        terms.append(over_plane(high, 1 << b))
    summed = total(terms)

    masks = range(1 << count)
    grads = ()
    part_width = half // PARTS
    for part in range(PARTS):
        columns = slice(part * part_width, (part + 1) * part_width)
        held = {0: jnp.concatenate([rows[:, columns] for rows in arrived], axis=0)}
        for v in masks[1:]:
            bit = v if DIRECT[part] else v & -v
            held[v] = over_plane(held[v ^ bit], bit)
        swapped = {}
        for v in masks:
            swapped[v] = over_core(held[v])
        grads = wgrad(
            place,
            shards,
            [held[v] for v in masks],
            [swapped[reverse_bits(v, count)] for v in masks],
            gate_rows,
            up_rows,
            part,
            PARTS,
            grads,
        )
    gate_wgrad, up_wgrad = grads

    blocks = summed.reshape(groups, 2 * capacity, half)
    back = [blocks[0]]
    for k in range(1, groups):
        back.append(over_expert(blocks[k], k))
    combined = lax.dot_general(
        selection, jnp.concatenate(back, axis=0), (((1,), (0,)), ((), ())),
        preferred_element_type=jnp.float32,
    ).astype(jnp.bfloat16)
    kept = combined[:token_count]
    got = over_core(combined[token_count:])
    token_grad = jnp.concatenate([by_core(kept, got), by_core(got, kept)], axis=1)
    return (token_grad, gate_wgrad[None], up_wgrad[None])


def solution(mesh):
    placed = (
        P(("expert", "shard"), None),
        P(("expert", "shard"), None),
        P("expert", None, "shard"),
        P("expert", None, "shard"),
        P("expert", None, "shard"),
        P("expert", None, "shard"),
        P("expert", None, "shard"),
    )

    return jax.shard_map(
        on_device,
        mesh=mesh,
        in_specs=placed,
        out_specs=(
            P(("expert", "shard"), None),
            P("expert", None, "shard"),
            P("expert", None, "shard"),
        ),
        check_vma=False,
    )
```
